32 devices in a mesh: cells: 16 (over z, y, x), faces: 2 (over core).
Axes of the slice: x: 2, y: 2, z: 4, core: 2. Of those that a mesh axis runs over, the one named last changes fastest.
Arguments:
- flow_state: float32 [4, 131072], P(None, 'cells'), may hold values from -6 to 6
- source_term: float32 [4, 131072], P(None, 'cells'), may hold values from -24 to 24
- volume_rate: float32 [131072], P('cells'), may hold values from 0.5 to 4
- face_normal: float32 [3, 393216], P(None, ('cells', 'faces')), may hold values from -3 to 3
- face_owner: int32 [393216], P(('cells', 'faces')), may hold values from 0 to 8191, as said below
- face_neighbour: int32 [393216], P(('cells', 'faces')), may hold values from 0 to 9727, as said below
- face_count: int32 [32], P(('cells', 'faces')), may hold values from 1536 to 12288, as said below
- send_list: int32 [96, 256], P('cells'), may hold values from 0 to 8191
- halo_count: int32 [96], P('cells'), may hold values from 64 to 256, as said below
Outputs:
- solution_field: float32 [4, 131072], P(None, 'cells')
- residual: float32 [4, 131072], P(None, 'cells')
The draws below stay inside these ranges and needn't reach their ends.
Inputs may be any that keep to these rules, and one draw needn't show every extreme that they name: `face_owner`: A local cell of the slot's partition; with s = g mod 12288 and t = s // 192, it lies in 128 * t to 128 * t + 127. `face_neighbour`: with s and t as for face_owner: below 8192 a local cell (128 * t + d) mod 8192 with d in 0 to 255; otherwise 8192 plus a halo slot of the slot's partition in (t mod (6)) * 256 to that plus 256 - 1. Live slots of a block are its first face_count slots; in every draw some block has all 12288 slots live. `send_list`: entries at or past the list's count are unused. `halo_count`: every partition has one list with exactly 256 entries.
All inputs are finite; a program needn't handle non-finite values.
Results may differ from the reference program's by a relative error of at most 0.0003.
Values sent between devices are 32-bit elements; how exact they have to be, the bound alone decides.
A program may use at most 64 MiB of HBM per device.

```python
import math
import jax
import jax.numpy as jnp
from jax import lax

CELLS_DEV = 8192
HALO = 256
NEIGH = 3
ITERS = 2
BLOCK = 4
TILES = 64
HWIN = 256
PARTITIONS = 16
SPLIT = 2
GROUPS = 32
FACE_SLOTS = 12288
CELLS = 131072
FACES = 393216


def draw_face_count(key, part):
    drawn_counts = jax.random.randint(key, (GROUPS,), FACE_SLOTS // 8, FACE_SLOTS + 1)
    chosen = jax.random.randint(jax.random.fold_in(key, 7), (), 0, GROUPS)
    return jnp.where(jnp.arange(GROUPS) == chosen, FACE_SLOTS, drawn_counts).astype(jnp.int32)


def draw_halo_count(key, part):
    list_total = 2 * NEIGH
    drawn_counts = jax.random.randint(key, (PARTITIONS, list_total), HALO // 4, HALO + 1)
    chosen = jax.random.randint(jax.random.fold_in(key, 11), (PARTITIONS, 1), 0, list_total)
    filled = jnp.where(jnp.arange(list_total)[None, :] == chosen, HALO, drawn_counts)
    return filled.reshape(PARTITIONS * list_total).astype(jnp.int32)


def tile_of_slot():
    slot_ids = jnp.arange(FACES, dtype=jnp.int32) % FACE_SLOTS
    return slot_ids // (FACE_SLOTS // TILES)


def draw_face_owner(key, part):
    tile_ids = tile_of_slot()
    offset = jax.random.randint(jax.random.fold_in(key, 21), (FACES,), 0, 128)
    return (tile_ids * 128 + offset).astype(jnp.int32)


def draw_face_neighbour(key, part):
    tile_ids = tile_of_slot()
    window_count = 2 * NEIGH * HALO // HWIN
    local_offset = jax.random.randint(jax.random.fold_in(key, 31), (FACES,), 0, 256)
    local_cell = (tile_ids * 128 + local_offset) % CELLS_DEV
    halo_offset = jax.random.randint(jax.random.fold_in(key, 37), (FACES,), 0, HWIN)
    halo_cell = CELLS_DEV + tile_ids % window_count * HWIN + halo_offset
    pick = jax.random.randint(jax.random.fold_in(key, 41), (FACES,), 0, 10)
    return jnp.where(pick < 3, halo_cell, local_cell).astype(jnp.int32)


def with_ends(values, key, least, high):
    place = [jax.random.randint(jax.random.fold_in(key, axis), (), 0, length) for axis, length in enumerate(values.shape)]
    main_axis = values.shape.index(max(values.shape))
    next_to = place[:main_axis] + [(place[main_axis] + 1) % values.shape[main_axis]] + place[main_axis + 1:]
    return values.at[tuple(place)].set(least).at[tuple(next_to)].set(high)


def shard_levels(stream_key, shape, shards, low, largest):
    loudness = 1.0
    for position, shards_of in shards:
        heights = jax.random.uniform(jax.random.fold_in(jax.random.fold_in(stream_key, 6), position), (shards_of,), jnp.float32, low / len(shards), largest / len(shards))
        loudness = loudness * jnp.repeat(jnp.exp(heights), shape[position] // shards_of).reshape((-1,) + (1,) * (len(shape) - 1 - position))
    return loudness


def bell_draw(stream_key, extent, width, limit, shards=(), kind=jnp.bfloat16):
    drawn = jax.random.normal(stream_key, extent, jnp.float32) * width
    if len(shards) > 0:
        drawn = shard_levels(stream_key, extent, shards, -0.22, 0.18) * drawn
    return jnp.clip(drawn, min=-limit, max=limit).astype(kind)


def setup_inputs(seed: int = 0) -> dict:
    key_list = jax.random.split(jax.random.key(seed), 10)
    return {
        "flow_state": bell_draw(key_list[0], (BLOCK, CELLS), 1.0, 6.0, ((1, 16),), jnp.float32),
        "source_term": bell_draw(key_list[1], (BLOCK, CELLS), 4.0, 24.0, ((1, 16),), jnp.float32),
        "volume_rate": jnp.clip(jnp.exp(math.log(4.0) - 2.0794415 * jax.random.uniform(key_list[2], (CELLS,), jnp.float32) ** shard_levels(key_list[2], (CELLS,), ((0, 16),), -0.2, 0.2)), 0.5, 4.0),
        "face_normal": bell_draw(key_list[3], (3, FACES), 0.5, 3.0, ((1, 32),), jnp.float32),
        "face_owner": draw_face_owner(jax.random.fold_in(key_list[9], 71), 0),
        "face_neighbour": draw_face_neighbour(jax.random.fold_in(key_list[9], 71), 0),
        "face_count": draw_face_count(jax.random.fold_in(key_list[9], 71), 0),
        "send_list": with_ends(jax.random.randint(key_list[7], (PARTITIONS * 2 * NEIGH, HALO), 0, CELLS_DEV), jax.random.fold_in(key_list[7], 1), 0, CELLS_DEV - 1).astype(jnp.int32),
        "halo_count": draw_halo_count(jax.random.fold_in(key_list[9], 71), 0),
    }


def shift_table():
    return jnp.array([which + 1 for which in range(NEIGH)] + [-(which + 1) for which in range(NEIGH)], jnp.int32)

def reference(flow_state, source_term, volume_rate, face_normal, face_owner, face_neighbour, face_count, send_list, halo_count):
    list_total = 2 * NEIGH
    face_ids = jnp.arange(FACES, dtype=jnp.int32)
    partition = face_ids // (FACE_SLOTS * SPLIT)
    is_live = (face_ids % FACE_SLOTS < face_count[face_ids // FACE_SLOTS]).astype(jnp.float32)
    owner_global = partition * CELLS_DEV + face_owner
    is_local = face_neighbour < CELLS_DEV
    halo_pos = jnp.maximum(face_neighbour - CELLS_DEV, 0)
    which_list = halo_pos // HALO
    which_slot = halo_pos % HALO
    sender = (partition - shift_table()[which_list]) % PARTITIONS
    list_row = sender * list_total + which_list
    sent_cell = send_list[list_row, which_slot]
    halo_live = which_slot < halo_count[list_row]
    neighbour_global = jnp.where(is_local, partition * CELLS_DEV + face_neighbour, sender * CELLS_DEV + sent_cell)
    neighbour_weight = jnp.where(is_local | halo_live, 1.0, 0.0).astype(jnp.float32)
    local_weight = is_local.astype(jnp.float32)
    sink_index = jnp.where(is_local, neighbour_global, CELLS)
    index_both = jnp.concatenate([owner_global, sink_index])

    def to_cells(owner_values, neighbour_values):
        stacked = jnp.concatenate([owner_values, neighbour_values], axis=1).T
        summed = jax.ops.segment_sum(stacked, index_both, num_segments=CELLS + 1)
        return summed[:CELLS].T
    left_state = flow_state[:, owner_global]
    right_state = flow_state[:, neighbour_global] * neighbour_weight
    normal_speed = 0.5 * lax.optimization_barrier(jnp.sum(face_normal * (left_state[:3] + right_state[:3]), axis=0))
    normal_size = jnp.sqrt(lax.optimization_barrier(jnp.sum(face_normal * face_normal, axis=0)))
    wave_speed = jnp.abs(normal_speed) + 2.0 * normal_size
    owner_terms = 0.5 * jnp.concatenate([normal_speed[None], face_normal, wave_speed[None]], axis=0) * is_live
    neighbour_terms = jnp.concatenate([-0.5 * normal_speed[None], -0.5 * face_normal, 0.5 * wave_speed[None]], axis=0) * (is_live * local_weight)
    block_terms = to_cells(owner_terms, neighbour_terms)
    velocity_diag = volume_rate + block_terms[0] + block_terms[4]
    pressure_diag = volume_rate + block_terms[4]
    coupling = block_terms[1:4]
    schur = pressure_diag - lax.optimization_barrier(jnp.sum(coupling * coupling, axis=0)) / velocity_diag

    def precondition(vector_in):
        pressure = (vector_in[3] - lax.optimization_barrier(jnp.sum(coupling * vector_in[:3], axis=0)) / velocity_diag) / schur
        velocity = (vector_in[:3] - coupling * pressure) / velocity_diag
        return jnp.concatenate([velocity, pressure[None]], axis=0)

    def apply_matrix(vector_in):
        left_side = vector_in[:, owner_global]
        right_side = vector_in[:, neighbour_global] * neighbour_weight
        face_sum = left_side + right_side
        central = jnp.concatenate([normal_speed * face_sum[:3] + face_normal * face_sum[3], lax.optimization_barrier(jnp.sum(face_normal * face_sum[:3], axis=0))[None]], axis=0)
        face_flux = (0.5 * central - 0.5 * wave_speed * (right_side - left_side)) * is_live
        return volume_rate * vector_in + to_cells(face_flux, -face_flux * local_weight)
    solution_field = jnp.zeros_like(source_term)
    residual = source_term
    shadow = source_term
    direction = source_term
    rho_now = jnp.sum(shadow * residual)
    for iteration in range(ITERS):
        pre_dir = precondition(direction)
        image = apply_matrix(pre_dir)
        step_alpha = rho_now / jnp.sum(shadow * image)
        middle = residual - step_alpha * image
        pre_mid = precondition(middle)
        second = apply_matrix(pre_mid)
        step_omega = jnp.sum(second * middle) / jnp.sum(second * second)
        solution_field = solution_field + step_alpha * pre_dir + step_omega * pre_mid
        residual = middle - step_omega * second
        if iteration + 1 < ITERS:
            rho_next = jnp.sum(shadow * residual)
            ratio_beta = rho_next / rho_now * (step_alpha / step_omega)
            direction = residual + ratio_beta * (direction - step_omega * image)
            rho_now = rho_next
    return (solution_field, residual)
```

```python
import functools

import jax
import jax.numpy as jnp
from jax import lax
from jax.experimental import pallas as pl
from jax.experimental.pallas import tpu as pltpu
from jax.sharding import PartitionSpec as P

ITERS = 2
LANES = 128
MESH = pl.DeviceIdType.MESH
F32 = jnp.float32
BF16 = jnp.bfloat16


def take_lanes(source, index):
    return jnp.take_along_axis(source, index, axis=1, mode="promise_in_bounds")


def split(value):
    high = value.astype(BF16).astype(F32)
    return high, value - high


def kernel(
    parts,
    cores,
    count_ref,
    flow_ref,
    source_ref,
    volume_ref,
    normal_ref,
    owner_ref,
    neighbour_ref,
    list_ref,
    halo_count_ref,
    solution_ref,
    residual_ref,
    own_lane,
    right_lane,
    right_kind,
    own_row,
    local_row,
    face_u,
    face_s,
    face_n,
    signed_hot,
    plain_hot,
    flux_rows,
    size_rows,
    cell_rows,
    size_cells,
    fields,
    halo_rows,
    blocks,
    vecs,
    pair_out,
    pair_in,
    halo_out,
    halo_in,
    dot_out,
    dot_in,
    pair_send,
    pair_recv,
    halo_send,
    halo_recv,
    dot_send,
    dot_recv,
):
    me = lax.axis_index("cells")
    core = lax.axis_index("faces")
    other = (core + 1) % cores
    tiles = volume_ref.shape[0]
    pairs = tiles // 2
    groups = pairs // 8
    cells = tiles * LANES
    lists = halo_in.shape[1]
    lists_here = lists // cores
    width = list_ref.shape[2] * list_ref.shape[1]

    barrier = pltpu.get_barrier_semaphore()
    for step in range(1, parts * cores):
        number = (me * cores + core + step) % (parts * cores)
        pl.semaphore_signal(
            barrier,
            inc=1,
            device_id={"cells": number // cores, "faces": number % cores},
            device_id_type=MESH,
        )

    lane = lax.broadcasted_iota(jnp.int32, (pairs, LANES), 1)
    pair_id = lax.broadcasted_iota(jnp.int32, (pairs, LANES), 0)
    late = lane >= LANES // 2
    count = count_ref[0]
    for j in range(3):
        tile = 2 * pair_id + (0 if j == 0 else 1)
        if j == 1:
            tile = 2 * pair_id + late.astype(jnp.int32)
        owner = owner_ref[pl.ds(j, pairs, stride=3), :]
        beside = neighbour_ref[pl.ds(j, pairs, stride=3), :]
        live = (3 * pair_id + j) * LANES + lane < count
        is_local = beside < cells
        column = beside - tile * LANES
        column = jnp.where(column < 0, column + cells, column)
        slot = beside - cells - (tile % lists) * width
        place = jnp.where(is_local, column, slot)
        upper = place >= LANES
        own = owner - tile * LANES
        own_lane[j] = own
        right_lane[j] = jnp.where(upper, place - LANES, place)
        right_kind[j] = jnp.where(is_local, 0, 2) + upper.astype(jnp.int32)
        own_row[j] = jnp.where(live, own, -1)
        local_row[j] = jnp.where(live & is_local, column, -1)

    def start_halo(turn, field):
        row8 = lax.broadcasted_iota(jnp.int32, (8, LANES), 0)
        for i in range(lists_here):
            which = core * lists_here + i
            rows = []
            wanted = list_ref[which]
            limit = halo_count_ref[which]
            for b in range(4):
                for half in range(2):
                    cell = jnp.broadcast_to(wanted[half : half + 1], (8, LANES))
                    row = cell // LANES
                    col = cell - row * LANES
                    found = jnp.zeros((8, LANES), F32)
                    for g in range(tiles // 8):
                        got = take_lanes(field(b, g), col)
                        found = jnp.where(row == row8 + 8 * g, got, found)
                    found = jnp.sum(found, axis=0, keepdims=True)
                    used = (
                        lax.broadcasted_iota(jnp.int32, (1, LANES), 1) + half * LANES < limit
                    )
                    rows.append(jnp.where(used, found, 0.0))
            halo_out[turn, i] = jnp.concatenate(rows, axis=0)
        for i in range(lists_here):
            target = (me + (1 - 2 * core) * (i + 1) + parts) % parts
            for c in range(cores):
                pltpu.make_async_remote_copy(
                    src_ref=halo_out.at[turn, i],
                    dst_ref=halo_in.at[turn, core * lists_here + i],
                    send_sem=halo_send.at[turn],
                    recv_sem=halo_recv.at[turn],
                    device_id={"cells": target, "faces": c},
                    device_id_type=MESH,
                ).start()

    def wait_halo(turn):
        pltpu.make_async_copy(halo_in.at[turn], halo_in.at[turn], halo_recv.at[turn]).wait()
        return [halo_in[turn, k] for k in range(lists)]

    def start_pair(turn, rows):
        copy = pltpu.make_async_remote_copy(
            src_ref=pair_out.at[turn, pl.ds(0, rows)],
            dst_ref=pair_in.at[turn, pl.ds(0, rows)],
            send_sem=pair_send.at[turn],
            recv_sem=pair_recv.at[turn],
            device_id={"cells": me, "faces": other},
            device_id_type=MESH,
        )
        copy.start()
        return copy

    def start_dots(turn, partials):
        rows = [
            jnp.sum(p.reshape(tiles // 8, 8, LANES).sum(axis=0), axis=0, keepdims=True)
            for p in partials
        ]
        rows.append(jnp.zeros((8 - len(rows), LANES), F32))
        packed = jnp.concatenate(rows, axis=0)
        dot_out[turn] = packed
        dot_in[turn, me] = packed
        for step in range(1, parts):
            pltpu.make_async_remote_copy(
                src_ref=dot_out.at[turn],
                dst_ref=dot_in.at[turn, me],
                send_sem=dot_send.at[turn],
                recv_sem=dot_recv.at[turn],
                device_id={"cells": (me + step) % parts, "faces": core},
                device_id_type=MESH,
            ).start()

    def wait_dots(turn, number):
        part = dot_in.at[turn, pl.ds(0, parts - 1)]
        pltpu.make_async_copy(part, part, dot_recv.at[turn]).wait()
        total = dot_in[turn, 0]
        for q in range(1, parts):
            total = total + dot_in[turn, q]
        total = jnp.sum(total, axis=1, keepdims=True)
        return [jnp.broadcast_to(total[d : d + 1], (1, LANES)) for d in range(number)]

    def put_field(values, halos):
        for b, value in enumerate(values):
            fields[b, pl.ds(0, tiles), :] = value
            fields[b, pl.ds(tiles, 1), :] = value[0:1]
        period = halo_rows.shape[0] // 8
        for t in range(period):
            halo_rows[pl.ds(t, 8, stride=period), :] = halos[t % lists]

    def sides(g, j, b):
        period = halo_rows.shape[0] // 8
        here = pl.multiple_of(g * 8, 8)
        left_at = own_lane[j, pl.ds(here, 8), :]
        right_at = right_lane[j, pl.ds(here, 8), :]
        kind = right_kind[j, pl.ds(here, 8), :]

        def of_tile(odd):
            first = 16 * g + odd
            halo_first = (16 * g) % lists + odd
            low = fields[b, pl.ds(first, 8, stride=2), :]
            high = fields[b, pl.ds(first + 1, 8, stride=2), :]
            halo_low = halo_rows[pl.ds(2 * b * period + halo_first, 8, stride=2), :]
            halo_high = halo_rows[pl.ds((2 * b + 1) * period + halo_first, 8, stride=2), :]
            left = take_lanes(low, left_at)
            right = jnp.where(
                kind < 2,
                jnp.where(kind == 0, take_lanes(low, right_at), take_lanes(high, right_at)),
                jnp.where(
                    kind == 2, take_lanes(halo_low, right_at), take_lanes(halo_high, right_at)
                ),
            )
            return left, right

        if j == 0:
            return of_tile(0)
        if j == 2:
            return of_tile(1)
        early = lax.broadcasted_iota(jnp.int32, (8, LANES), 1) < LANES // 2
        left_a, right_a = of_tile(0)
        left_b, right_b = of_tile(1)
        return jnp.where(early, left_a, left_b), jnp.where(early, right_a, right_b)

    def put_flux(ref, g, j, b, value):
        high, low = split(value)
        ref[j, pl.ds(64 * g + b, 8, stride=8), :] = high
        ref[j, pl.ds(64 * g + 4 + b, 8, stride=8), :] = low

    def scatter(rows_ref, hot_ref, cells_ref, u):
        start = pl.multiple_of(u * 8, 8)
        for odd in range(2):
            rows = jnp.concatenate(
                [rows_ref[odd, pl.ds(start, 8), :], rows_ref[odd + 1, pl.ds(start, 8), :]], axis=1
            ).astype(BF16)
            result = lax.dot_general(
                rows, hot_ref[2 * u + odd], (((1,), (1,)), ((), ())), preferred_element_type=F32
            )
            at = pl.ds(pl.multiple_of(start * 2 + odd * 8, 8), 8)
            cells_ref[0, at, :] = result[:, :LANES]
            cells_ref[1, at, :] = result[:, LANES:]

    def collect(cells_ref, b):
        def rows(first, side):
            return cells_ref[side, pl.ds(first, tiles, stride=8), :]

        low = rows(b, 0) + rows(4 + b, 0)
        high = rows(b, 1) + rows(4 + b, 1)
        high = jnp.concatenate([high[tiles - 1 :], high[: tiles - 1]], axis=0)
        return low + high

    def apply_matrix(turn, values, halos):
        put_field(values, halos)

        def group(g, carry):
            here = pl.multiple_of(g * 8, 8)
            for j in range(3):
                u = face_u[j, pl.ds(here, 8), :]
                s = face_s[j, pl.ds(here, 8), :]
                n = [face_n[i, j, pl.ds(here, 8), :] for i in range(3)]
                both = [sides(g, j, b) for b in range(4)]
                total = [left + right for left, right in both]
                jump = [s * (right - left) for left, right in both]
                for i in range(3):
                    put_flux(flux_rows, g, j, i, u * total[i] + n[i] * total[3] - jump[i])
                last = n[0] * total[0] + n[1] * total[1] + n[2] * total[2] - jump[3]
                put_flux(flux_rows, g, j, 3, last)
            for i in range(8):
                scatter(flux_rows, signed_hot, cell_rows, g * 8 + i)
            return carry

        lax.fori_loop(0, groups, group, 0)
        mine = [collect(cell_rows, b) for b in range(4)]
        for b in range(4):
            pair_out[turn, b * tiles : (b + 1) * tiles, :] = mine[b]
        copy = start_pair(turn, 4 * tiles)
        copy.wait_recv()
        volume = volume_ref[...]
        return [
            volume * values[b]
            + (
                pair_out[turn, b * tiles : (b + 1) * tiles, :]
                + pair_in[turn, b * tiles : (b + 1) * tiles, :]
            )
            for b in range(4)
        ]

    def precondition(w):
        rvd, rschur = blocks[0], blocks[1]
        n = [blocks[2 + i] for i in range(3)]
        pressure = (w[3] - (n[0] * w[0] + n[1] * w[1] + n[2] * w[2]) * rvd) * rschur
        return [(w[i] - n[i] * pressure) * rvd for i in range(3)] + [pressure]

    def load(which):
        return [vecs[which, b] for b in range(4)]

    def save(which, values):
        for b in range(4):
            vecs[which, b] = values[b]

    def dot(a, b):
        return a[0] * b[0] + a[1] * b[1] + a[2] * b[2] + a[3] * b[3]

    def saved_field(which):
        return lambda b, g: vecs[which, b, 8 * g : 8 * g + 8, :]

    PRE, IMAGE_M, TEMP = 0, 1, 2
    flow = [flow_ref[pl.ds(b, tiles, stride=4), :] for b in range(4)]
    source = [source_ref[pl.ds(b, tiles, stride=4), :] for b in range(4)]
    save(TEMP, flow)
    pl.semaphore_wait(barrier, parts * cores - 1)
    start_halo(0, saved_field(TEMP))
    start_dots(0, [dot(source, source)])

    cell_id = lax.broadcasted_iota(jnp.int32, (2 * LANES, LANES), 0)
    early_row = lax.broadcasted_iota(jnp.int32, (1, LANES), 1) < LANES // 2

    def build(u, carry):
        for odd in range(2):
            for half in range(2):
                j = odd + half
                own = own_row[j, pl.ds(u, 1), :]
                local = local_row[j, pl.ds(u, 1), :]
                if j == 1:
                    keep = early_row if odd == 0 else jnp.logical_not(early_row)
                    own = jnp.where(keep, own, -1)
                    local = jnp.where(keep, local, -1)
                own_hot = jnp.where(cell_id == own, 1.0, 0.0)
                local_hot = jnp.where(cell_id == local, 1.0, 0.0)
                lanes = slice(half * LANES, (half + 1) * LANES)
                signed_hot[2 * u + odd, :, lanes] = (own_hot - local_hot).astype(BF16)
                plain_hot[2 * u + odd, :, lanes] = (own_hot + local_hot).astype(BF16)
        return carry

    lax.fori_loop(0, pairs, build, 0)
    size_rows[...] = jnp.zeros_like(size_rows)

    put_field(flow, wait_halo(0))

    def face_terms(g, carry):
        here = pl.multiple_of(g * 8, 8)
        for j in range(3):
            n = [normal_ref[i, pl.ds(24 * g + j, 8, stride=3), :] for i in range(3)]
            both = [sides(g, j, b) for b in range(3)]
            total = [left + right for left, right in both]
            u = 0.5 * (n[0] * total[0] + n[1] * total[1] + n[2] * total[2])
            s = jnp.abs(u) + 2.0 * jnp.sqrt(n[0] * n[0] + n[1] * n[1] + n[2] * n[2])
            u, s = 0.5 * u, 0.5 * s
            n = [0.5 * n[i] for i in range(3)]
            face_u[j, pl.ds(here, 8), :] = u
            face_s[j, pl.ds(here, 8), :] = s
            put_flux(flux_rows, g, j, 0, u)
            for i in range(3):
                face_n[i, j, pl.ds(here, 8), :] = n[i]
                put_flux(flux_rows, g, j, 1 + i, n[i])
            put_flux(size_rows, g, j, 0, s)
        for i in range(8):
            scatter(flux_rows, signed_hot, cell_rows, g * 8 + i)
            scatter(size_rows, plain_hot, size_cells, g * 8 + i)
        return carry

    lax.fori_loop(0, groups, face_terms, 0)
    for b in range(4):
        pair_out[0, b * tiles : (b + 1) * tiles, :] = collect(cell_rows, b)
    pair_out[0, 4 * tiles : 5 * tiles, :] = collect(size_cells, 0)
    start_pair(0, 5 * tiles).wait_recv()
    sums = [
        pair_out[0, b * tiles : (b + 1) * tiles, :] + pair_in[0, b * tiles : (b + 1) * tiles, :]
        for b in range(5)
    ]
    volume = volume_ref[...]
    rvd = 1.0 / (volume + sums[0] + sums[4])
    coupling = sums[1:4]
    norm = coupling[0] * coupling[0] + coupling[1] * coupling[1] + coupling[2] * coupling[2]
    blocks[0] = rvd
    blocks[1] = 1.0 / (volume + sums[4] - norm * rvd)
    for i in range(3):
        blocks[2 + i] = coupling[i]

    def combine(a, scale, b):
        return [x + scale * y for x, y in zip(a, b)]

    residual = source
    direction = source
    pre_dir = precondition(direction)
    save(PRE, pre_dir)
    start_halo(1, saved_field(PRE))
    (rho,) = wait_dots(0, 1)
    halo_dir = wait_halo(1)
    halo_res = halo_dir
    answer = None
    for iteration in range(ITERS):
        final = iteration + 1 == ITERS
        turn = 1 + 2 * iteration
        image = apply_matrix(turn, pre_dir, halo_dir)
        start_dots(turn, [dot(source, image)])
        pre_image = precondition(image)
        save(IMAGE_M, pre_image)
        start_halo(turn + 1, saved_field(IMAGE_M))
        pre_res = pre_dir if iteration == 0 else precondition(residual)
        (shadow_image,) = wait_dots(turn, 1)
        alpha = rho / shadow_image
        middle = combine(residual, -alpha, image)
        pre_mid = combine(pre_res, -alpha, pre_image)
        halo_image = wait_halo(turn + 1)
        halo_mid = combine(halo_res, -alpha, halo_image)
        second = apply_matrix(turn + 1, pre_mid, halo_mid)
        start_dots(
            turn + 1,
            [dot(second, middle), dot(second, second), dot(source, middle), dot(source, second)],
        )
        if not final:
            pre_second = precondition(second)
            save(TEMP, pre_second)
            start_halo(turn + 2, saved_field(TEMP))
        second_mid, second_sq, shadow_mid, shadow_second = wait_dots(turn + 1, 4)
        omega = second_mid / second_sq
        step = combine([alpha * v for v in pre_dir], omega, pre_mid)
        answer = step if answer is None else [a + s for a, s in zip(answer, step)]
        residual = combine(middle, -omega, second)
        if not final:
            rho_next = shadow_mid - omega * shadow_second
            beta = rho_next / rho * (alpha / omega)
            rho = rho_next
            direction = combine(residual, beta, combine(direction, -omega, image))
            pre_dir = precondition(direction)
            halo_second = wait_halo(turn + 2)
            halo_res = combine(halo_mid, -omega, halo_second)
            halo_dir = combine(halo_res, beta, combine(halo_dir, -omega, halo_image))
    for b in range(4):
        solution_ref[pl.ds(b, tiles, stride=4), :] = answer[b]
        residual_ref[pl.ds(b, tiles, stride=4), :] = residual[b]

    for turn in range(halo_in.shape[0]):
        pltpu.make_async_copy(halo_in.at[turn], halo_in.at[turn], halo_send.at[turn]).wait()
    for turn in range(pair_in.shape[0]):
        part = pair_out.at[turn, pl.ds(0, (5 if turn == 0 else 4) * tiles)]
        pltpu.make_async_copy(part, part, pair_send.at[turn]).wait()
        part = dot_in.at[turn, pl.ds(0, parts - 1)]
        pltpu.make_async_copy(part, part, dot_send.at[turn]).wait()


def body(
    flow_state,
    source_term,
    volume_rate,
    face_normal,
    face_owner,
    face_neighbour,
    face_count,
    send_list,
    halo_count,
):
    parts = lax.axis_size("cells")
    cores = lax.axis_size("faces")
    cells = flow_state.shape[1]
    tiles = cells // LANES
    pairs = tiles // 2
    face_rows = face_owner.shape[0] // LANES
    lists, width = send_list.shape
    period = -(-(lists + 16) // 8) * 8
    turns = 1 + 2 * ITERS

    def by_tile(field):
        return field.reshape(4, tiles, LANES).transpose(1, 0, 2).reshape(4 * tiles, LANES)

    def by_component(field):
        return field.reshape(tiles, 4, LANES).transpose(1, 0, 2).reshape(4, cells)

    vmem = pl.BlockSpec(memory_space=pltpu.VMEM)
    smem = pl.BlockSpec(memory_space=pltpu.SMEM)
    ints = pltpu.VMEM((3, pairs, LANES), jnp.int32)
    floats = pltpu.VMEM((3, pairs, LANES), F32)
    hot = pltpu.VMEM((tiles, 2 * LANES, 2 * LANES), BF16)
    out = jax.ShapeDtypeStruct((4 * tiles, LANES), F32)
    solved, left = pl.pallas_call(
        functools.partial(kernel, parts, cores),
        out_shape=(out, out),
        in_specs=[smem] + [vmem] * 7 + [smem],
        out_specs=(vmem, vmem),
        scratch_shapes=[
            ints,
            ints,
            ints,
            ints,
            ints,
            floats,
            floats,
            pltpu.VMEM((3, 3, pairs, LANES), F32),
            hot,
            hot,
            pltpu.VMEM((3, 8 * pairs, LANES), F32),
            pltpu.VMEM((3, 8 * pairs, LANES), F32),
            pltpu.VMEM((2, 8 * tiles, LANES), F32),
            pltpu.VMEM((2, 8 * tiles, LANES), F32),
            pltpu.VMEM((4, tiles + 8, LANES), F32),
            pltpu.VMEM((8 * period, LANES), F32),
            pltpu.VMEM((5, tiles, LANES), F32),
            pltpu.VMEM((3, 4, tiles, LANES), F32),
            pltpu.VMEM((turns, 5 * tiles, LANES), F32),
            pltpu.VMEM((turns, 5 * tiles, LANES), F32),
            pltpu.VMEM((turns, lists // cores, 8, LANES), F32),
            pltpu.VMEM((turns, lists, 8, LANES), F32),
            pltpu.VMEM((turns, 8, LANES), F32),
            pltpu.VMEM((turns, parts, 8, LANES), F32),
        ]
        + [pltpu.SemaphoreType.DMA((turns,))] * 6,
        compiler_params=pltpu.CompilerParams(
            collective_id=0, has_side_effects=True, vmem_limit_bytes=56 * 1024 * 1024
        ),
    )(
        face_count,
        by_tile(flow_state),
        by_tile(source_term),
        volume_rate.reshape(tiles, LANES),
        face_normal.reshape(3, face_rows, LANES),
        face_owner.reshape(face_rows, LANES),
        face_neighbour.reshape(face_rows, LANES),
        send_list.reshape(lists, width // LANES, LANES),
        halo_count,
    )
    return by_component(solved), by_component(left)


def solution(mesh):
    in_specs = (
        P(None, "cells"),
        P(None, "cells"),
        P("cells"),
        P(None, ("cells", "faces")),
        P(("cells", "faces")),
        P(("cells", "faces")),
        P(("cells", "faces")),
        P("cells", None),
        P("cells"),
    )
    out_specs = (P(None, "cells"), P(None, "cells"))
    return jax.shard_map(body, mesh=mesh, in_specs=in_specs, out_specs=out_specs, check_vma=False)
```

```python
import functools

import jax
import jax.numpy as jnp
from jax import lax
from jax.experimental import pallas as pl
from jax.experimental.pallas import tpu as pltpu
from jax.sharding import PartitionSpec as P

ITERS = 2
LANES = 128
MESH = pl.DeviceIdType.MESH
F32 = jnp.float32
BF16 = jnp.bfloat16


def take_lanes(source, index):
    return jnp.take_along_axis(source, index, axis=1, mode="promise_in_bounds")


def split(value):
    high = value.astype(BF16).astype(F32)
    return high, value - high


def kernel(
    parts,
    cores,
    count_ref,
    flow_hbm,
    source_hbm,
    volume_hbm,
    normal_hbm,
    owner_hbm,
    neighbour_hbm,
    list_ref,
    halo_count_ref,
    solution_ref,
    residual_ref,
    flow_ref,
    source_ref,
    volume_ref,
    normal_ref,
    owner_ref,
    neighbour_ref,
    input_sem,
    own_lane,
    right_lane,
    right_kind,
    own_row,
    local_row,
    face_u,
    face_s,
    face_n,
    signed_hot,
    plain_hot,
    flux_rows,
    size_rows,
    cell_rows,
    size_cells,
    fields,
    halo_rows,
    blocks,
    vecs,
    pair_out,
    pair_in,
    halo_out,
    halo_in,
    dot_out,
    dot_in,
    pair_send,
    pair_recv,
    halo_send,
    halo_recv,
    dot_send,
    dot_recv,
):
    me = lax.axis_index("cells")
    core = lax.axis_index("faces")
    other = (core + 1) % cores
    tiles = volume_ref.shape[0]
    pairs = tiles // 2
    groups = pairs // 8
    cells = tiles * LANES
    lists = halo_in.shape[1]
    lists_here = lists // cores
    width = list_ref.shape[1] * LANES

    def fetched(number, source, target):
        copy = pltpu.make_async_copy(source, target, input_sem.at[number])
        copy.start()
        return copy

    copies = [
        fetched(0, owner_hbm, owner_ref),
        fetched(1, neighbour_hbm, neighbour_ref),
        fetched(2, flow_hbm, flow_ref),
        fetched(4, source_hbm, source_ref),
        fetched(5, volume_hbm, volume_ref),
    ]
    normals = [fetched(3, normal_hbm, normal_ref)]

    barrier = pltpu.get_barrier_semaphore()
    for step in range(1, parts * cores):
        number = (me * cores + core + step) % (parts * cores)
        pl.semaphore_signal(
            barrier,
            inc=1,
            device_id={"cells": number // cores, "faces": number % cores},
            device_id_type=MESH,
        )

    lane = lax.broadcasted_iota(jnp.int32, (pairs, LANES), 1)
    pair_id = lax.broadcasted_iota(jnp.int32, (pairs, LANES), 0)
    late = lane >= LANES // 2
    count = count_ref[0]
    for copy in copies:
        copy.wait()
    for j in range(3):
        tile = 2 * pair_id + (0 if j == 0 else 1)
        if j == 1:
            tile = 2 * pair_id + late.astype(jnp.int32)
        owner = owner_ref[pl.ds(j, pairs, stride=3), :]
        beside = neighbour_ref[pl.ds(j, pairs, stride=3), :]
        live = (3 * pair_id + j) * LANES + lane < count
        is_local = beside < cells
        column = beside - tile * LANES
        column = jnp.where(column < 0, column + cells, column)
        slot = beside - cells - (tile % lists) * width
        place = jnp.where(is_local, column, slot)
        upper = place >= LANES
        own = owner - tile * LANES
        own_lane[j] = own
        right_lane[j] = jnp.where(upper, place - LANES, place)
        right_kind[j] = jnp.where(is_local, 0, 2) + upper.astype(jnp.int32)
        own_row[j] = jnp.where(live, own, -1).astype(F32)
        local_row[j] = jnp.where(live & is_local, column, -1).astype(F32)

    def start_halo(turn, field):
        row8 = lax.broadcasted_iota(jnp.int32, (8, LANES), 0)
        for i in range(lists_here):
            which = core * lists_here + i
            rows = []
            wanted = list_ref[which]
            limit = halo_count_ref[which]
            for b in range(4):
                for half in range(2):
                    cell = jnp.broadcast_to(wanted[half : half + 1], (8, LANES))
                    row = cell // LANES
                    col = cell - row * LANES
                    found = jnp.zeros((8, LANES), F32)
                    for g in range(tiles // 8):
                        got = take_lanes(field(b, g), col)
                        found = jnp.where(row == row8 + 8 * g, got, found)
                    found = jnp.sum(found, axis=0, keepdims=True)
                    used = (
                        lax.broadcasted_iota(jnp.int32, (1, LANES), 1) + half * LANES < limit
                    )
                    rows.append(jnp.where(used, found, 0.0))
            halo_out[turn, i] = jnp.concatenate(rows, axis=0)
        for i in range(lists_here):
            target = (me + (1 - 2 * core) * (i + 1) + parts) % parts
            for c in range(cores):
                pltpu.make_async_remote_copy(
                    src_ref=halo_out.at[turn, i],
                    dst_ref=halo_in.at[turn, core * lists_here + i],
                    send_sem=halo_send.at[turn],
                    recv_sem=halo_recv.at[turn],
                    device_id={"cells": target, "faces": c},
                    device_id_type=MESH,
                ).start()

    def wait_halo(turn):
        pltpu.make_async_copy(halo_in.at[turn], halo_in.at[turn], halo_recv.at[turn]).wait()
        return [halo_in[turn, k] for k in range(lists)]

    def start_pair(turn, rows):
        copy = pltpu.make_async_remote_copy(
            src_ref=pair_out.at[turn, pl.ds(0, rows)],
            dst_ref=pair_in.at[turn, pl.ds(0, rows)],
            send_sem=pair_send.at[turn],
            recv_sem=pair_recv.at[turn],
            device_id={"cells": me, "faces": other},
            device_id_type=MESH,
        )
        copy.start()
        return copy

    def start_dots(turn, partials):
        at = lax.broadcasted_iota(jnp.int32, (1, LANES), 1)
        packed = jnp.zeros((1, LANES), F32)
        for d, p in enumerate(partials):
            row = jnp.sum(p.reshape(tiles // 8, 8, LANES).sum(axis=0), axis=0, keepdims=True)
            packed = jnp.where(at == d, jnp.sum(row, axis=1, keepdims=True), packed)
        dot_out[turn] = packed
        dot_in[turn, me] = packed
        for step in range(1, parts):
            pltpu.make_async_remote_copy(
                src_ref=dot_out.at[turn],
                dst_ref=dot_in.at[turn, me],
                send_sem=dot_send.at[turn],
                recv_sem=dot_recv.at[turn],
                device_id={"cells": (me + step) % parts, "faces": core},
                device_id_type=MESH,
            ).start()

    def wait_dots(turn, number):
        part = dot_in.at[turn, pl.ds(0, parts - 1)]
        pltpu.make_async_copy(part, part, dot_recv.at[turn]).wait()
        total = dot_in[turn, 0]
        for q in range(1, parts):
            total = total + dot_in[turn, q]
        return [jnp.broadcast_to(total[:, d : d + 1], (1, LANES)) for d in range(number)]

    def put_field(values, halos):
        for b, value in enumerate(values):
            fields[b, pl.ds(0, tiles), :] = value
            fields[b, pl.ds(tiles, 1), :] = value[0:1]
        period = halo_rows.shape[0] // 8
        for t in range(period):
            halo_rows[pl.ds(t, 8, stride=period), :] = halos[t % lists]

    def sides(g, j, b):
        period = halo_rows.shape[0] // 8
        here = pl.multiple_of(g * 8, 8)
        left_at = own_lane[j, pl.ds(here, 8), :]
        right_at = right_lane[j, pl.ds(here, 8), :]
        kind = right_kind[j, pl.ds(here, 8), :]

        def of_tile(odd):
            first = 16 * g + odd
            halo_first = (16 * g) % lists + odd
            low = fields[b, pl.ds(first, 8, stride=2), :]
            high = fields[b, pl.ds(first + 1, 8, stride=2), :]
            halo_low = halo_rows[pl.ds(2 * b * period + halo_first, 8, stride=2), :]
            halo_high = halo_rows[pl.ds((2 * b + 1) * period + halo_first, 8, stride=2), :]
            left = take_lanes(low, left_at)
            right = jnp.where(
                kind < 2,
                jnp.where(kind == 0, take_lanes(low, right_at), take_lanes(high, right_at)),
                jnp.where(
                    kind == 2, take_lanes(halo_low, right_at), take_lanes(halo_high, right_at)
                ),
            )
            return left, right

        if j == 0:
            return of_tile(0)
        if j == 2:
            return of_tile(1)
        early = lax.broadcasted_iota(jnp.int32, (8, LANES), 1) < LANES // 2
        left_a, right_a = of_tile(0)
        left_b, right_b = of_tile(1)
        return jnp.where(early, left_a, left_b), jnp.where(early, right_a, right_b)

    def put_flux(ref, g, j, b, value):
        high, low = split(value)
        ref[j, pl.ds(64 * g + b, 8, stride=8), :] = high
        ref[j, pl.ds(64 * g + 4 + b, 8, stride=8), :] = low

    def tile_rows(rows_ref, u, odd):
        at = pl.ds(pl.multiple_of(u * 8, 8), 8)
        return jnp.concatenate([rows_ref[odd, at, :], rows_ref[odd + 1, at, :]], axis=1).astype(BF16)

    def added(rows, hot):
        return lax.dot_general(
            rows, hot, (((1,), (1,)), ((), ())), preferred_element_type=F32
        )

    def scatter(u):
        for odd in range(2):
            result = added(tile_rows(flux_rows, u, odd), signed_hot[2 * u + odd])
            at = pl.ds(pl.multiple_of(u * 16 + odd * 8, 8), 8)
            cell_rows[0, at, :] = result[:, :LANES]
            cell_rows[1, at, :] = result[:, LANES:]

    def scatter_size(u):
        for odd in range(2):
            rows = tile_rows(size_rows, u, odd)
            at = pl.ds(pl.multiple_of(u * 16 + odd * 8, 8), 8)
            size_cells[0, at, :] = added(rows, plain_hot[2 * u + odd])
            size_cells[1, at, :] = -added(rows, signed_hot[2 * u + odd, LANES:, :])

    def collect(cells_ref, b):
        def rows(first, side):
            return cells_ref[side, pl.ds(first, tiles, stride=8), :]

        low = rows(b, 0) + rows(4 + b, 0)
        high = rows(b, 1) + rows(4 + b, 1)
        high = jnp.concatenate([high[tiles - 1 :], high[: tiles - 1]], axis=0)
        return low + high

    def apply_matrix(turn, values, halos):
        put_field(values, halos)

        def group(g, carry):
            here = pl.multiple_of(g * 8, 8)
            for j in range(3):
                u = face_u[j, pl.ds(here, 8), :]
                s = face_s[j, pl.ds(here, 8), :]
                n = [face_n[i, j, pl.ds(here, 8), :] for i in range(3)]
                both = [sides(g, j, b) for b in range(4)]
                total = [left + right for left, right in both]
                jump = [s * (right - left) for left, right in both]
                for i in range(3):
                    put_flux(flux_rows, g, j, i, u * total[i] + n[i] * total[3] - jump[i])
                last = n[0] * total[0] + n[1] * total[1] + n[2] * total[2] - jump[3]
                put_flux(flux_rows, g, j, 3, last)
            for i in range(8):
                scatter(g * 8 + i)
            return carry

        lax.fori_loop(0, groups, group, 0)
        mine = [collect(cell_rows, b) for b in range(4)]
        for b in range(4):
            pair_out[turn, b * tiles : (b + 1) * tiles, :] = mine[b]
        copy = start_pair(turn, 4 * tiles)
        copy.wait_recv()
        volume = volume_ref[...]
        return [
            volume * values[b]
            + (
                pair_out[turn, b * tiles : (b + 1) * tiles, :]
                + pair_in[turn, b * tiles : (b + 1) * tiles, :]
            )
            for b in range(4)
        ]

    def precondition(w):
        rvd, rschur = blocks[0], blocks[1]
        n = [blocks[2 + i] for i in range(3)]
        pressure = (w[3] - (n[0] * w[0] + n[1] * w[1] + n[2] * w[2]) * rvd) * rschur
        return [(w[i] - n[i] * pressure) * rvd for i in range(3)] + [pressure]

    def load(which):
        return [vecs[which, b] for b in range(4)]

    def save(which, values):
        for b in range(4):
            vecs[which, b] = values[b]

    def dot(a, b):
        return a[0] * b[0] + a[1] * b[1] + a[2] * b[2] + a[3] * b[3]

    def saved_field(which):
        return lambda b, g: vecs[which, b, 8 * g : 8 * g + 8, :]

    PRE, IMAGE_M, TEMP = 0, 1, 2
    flow = [flow_ref[pl.ds(b, tiles, stride=4), :] for b in range(4)]
    source = [source_ref[pl.ds(b, tiles, stride=4), :] for b in range(4)]
    pl.semaphore_wait(barrier, parts * cores - 1)
    start_halo(0, lambda b, g: flow_ref[pl.ds(32 * g + b, 8, stride=4), :])
    start_dots(0, [dot(source, source)])

    cell_id = lax.broadcasted_iota(jnp.int32, (LANES, LANES), 0).astype(F32).astype(BF16)
    early_row = lax.broadcasted_iota(jnp.int32, (1, LANES), 1) < LANES // 2
    one, zero = jnp.ones((), BF16), jnp.zeros((), BF16)

    def hot_of(row):
        return jnp.where(cell_id == row.astype(BF16), one, zero)

    def build(u, carry):
        for odd in range(2):
            for half in range(2):
                j = odd + half
                own = own_row[j, pl.ds(u, 1), :]
                local = local_row[j, pl.ds(u, 1), :]
                if j == 1:
                    keep = early_row if odd == 0 else jnp.logical_not(early_row)
                    own = jnp.where(keep, own, -1.0)
                    local = jnp.where(keep, local, -1.0)
                own_hot, local_hot = hot_of(own), hot_of(local)
                lanes = slice(half * LANES, (half + 1) * LANES)
                signed_hot[2 * u + odd, :LANES, lanes] = own_hot - local_hot
                signed_hot[2 * u + odd, LANES:, lanes] = -hot_of(local - LANES)
                plain_hot[2 * u + odd, :, lanes] = own_hot + local_hot
        return carry

    lax.fori_loop(0, pairs, build, 0)
    size_rows[...] = jnp.zeros_like(size_rows)
    for copy in normals:
        copy.wait()

    put_field(flow, wait_halo(0))

    def face_terms(g, carry):
        here = pl.multiple_of(g * 8, 8)
        for j in range(3):
            n = [normal_ref[i, pl.ds(24 * g + j, 8, stride=3), :] for i in range(3)]
            both = [sides(g, j, b) for b in range(3)]
            total = [left + right for left, right in both]
            u = 0.5 * (n[0] * total[0] + n[1] * total[1] + n[2] * total[2])
            s = jnp.abs(u) + 2.0 * jnp.sqrt(n[0] * n[0] + n[1] * n[1] + n[2] * n[2])
            u, s = 0.5 * u, 0.5 * s
            n = [0.5 * n[i] for i in range(3)]
            face_u[j, pl.ds(here, 8), :] = u
            face_s[j, pl.ds(here, 8), :] = s
            put_flux(flux_rows, g, j, 0, u)
            for i in range(3):
                face_n[i, j, pl.ds(here, 8), :] = n[i]
                put_flux(flux_rows, g, j, 1 + i, n[i])
            put_flux(size_rows, g, j, 0, s)
        for i in range(8):
            scatter(g * 8 + i)
            scatter_size(g * 8 + i)
        return carry

    lax.fori_loop(0, groups, face_terms, 0)
    for b in range(4):
        pair_out[0, b * tiles : (b + 1) * tiles, :] = collect(cell_rows, b)
    pair_out[0, 4 * tiles : 5 * tiles, :] = collect(size_cells, 0)
    start_pair(0, 5 * tiles).wait_recv()
    sums = [
        pair_out[0, b * tiles : (b + 1) * tiles, :] + pair_in[0, b * tiles : (b + 1) * tiles, :]
        for b in range(5)
    ]
    volume = volume_ref[...]
    rvd = 1.0 / (volume + sums[0] + sums[4])
    coupling = sums[1:4]
    norm = coupling[0] * coupling[0] + coupling[1] * coupling[1] + coupling[2] * coupling[2]
    blocks[0] = rvd
    blocks[1] = 1.0 / (volume + sums[4] - norm * rvd)
    for i in range(3):
        blocks[2 + i] = coupling[i]

    def combine(a, scale, b):
        return [x + scale * y for x, y in zip(a, b)]

    residual = source
    direction = source
    pre_dir = precondition(direction)
    save(PRE, pre_dir)
    start_halo(1, saved_field(PRE))
    (rho,) = wait_dots(0, 1)
    halo_dir = wait_halo(1)
    halo_res = halo_dir
    answer = None
    for iteration in range(ITERS):
        final = iteration + 1 == ITERS
        turn = 1 + 2 * iteration
        image = apply_matrix(turn, pre_dir, halo_dir)
        start_dots(turn, [dot(source, image)])
        pre_image = precondition(image)
        save(IMAGE_M, pre_image)
        start_halo(turn + 1, saved_field(IMAGE_M))
        pre_res = pre_dir if iteration == 0 else precondition(residual)
        (shadow_image,) = wait_dots(turn, 1)
        alpha = rho / shadow_image
        middle = combine(residual, -alpha, image)
        pre_mid = combine(pre_res, -alpha, pre_image)
        halo_image = wait_halo(turn + 1)
        halo_mid = combine(halo_res, -alpha, halo_image)
        second = apply_matrix(turn + 1, pre_mid, halo_mid)
        start_dots(
            turn + 1,
            [dot(second, middle), dot(second, second), dot(source, middle), dot(source, second)],
        )
        if not final:
            pre_second = precondition(second)
            save(TEMP, pre_second)
            start_halo(turn + 2, saved_field(TEMP))
        second_mid, second_sq, shadow_mid, shadow_second = wait_dots(turn + 1, 4)
        omega = second_mid / second_sq
        step = combine([alpha * v for v in pre_dir], omega, pre_mid)
        answer = step if answer is None else [a + s for a, s in zip(answer, step)]
        residual = combine(middle, -omega, second)
        if not final:
            rho_next = shadow_mid - omega * shadow_second
            beta = rho_next / rho * (alpha / omega)
            rho = rho_next
            direction = combine(residual, beta, combine(direction, -omega, image))
            pre_dir = precondition(direction)
            halo_second = wait_halo(turn + 2)
            halo_res = combine(halo_mid, -omega, halo_second)
            halo_dir = combine(halo_res, beta, combine(halo_dir, -omega, halo_image))
    for b in range(4):
        solution_ref[pl.ds(b, tiles, stride=4), :] = answer[b]
        residual_ref[pl.ds(b, tiles, stride=4), :] = residual[b]

    for turn in range(halo_in.shape[0]):
        pltpu.make_async_copy(halo_in.at[turn], halo_in.at[turn], halo_send.at[turn]).wait()
    for turn in range(pair_in.shape[0]):
        part = pair_out.at[turn, pl.ds(0, (5 if turn == 0 else 4) * tiles)]
        pltpu.make_async_copy(part, part, pair_send.at[turn]).wait()
        part = dot_in.at[turn, pl.ds(0, parts - 1)]
        pltpu.make_async_copy(part, part, dot_send.at[turn]).wait()


def body(
    flow_state,
    source_term,
    volume_rate,
    face_normal,
    face_owner,
    face_neighbour,
    face_count,
    send_list,
    halo_count,
):
    parts = lax.axis_size("cells")
    cores = lax.axis_size("faces")
    cells = flow_state.shape[1]
    tiles = cells // LANES
    pairs = tiles // 2
    face_rows = face_owner.shape[0] // LANES
    lists, width = send_list.shape
    period = -(-(lists + 16) // 8) * 8
    turns = 1 + 2 * ITERS

    def by_tile(field):
        return field.reshape(4, tiles, LANES).transpose(1, 0, 2).reshape(4 * tiles, LANES)

    def by_component(field):
        return field.reshape(tiles, 4, LANES).transpose(1, 0, 2).reshape(4, cells)

    vmem = pl.BlockSpec(memory_space=pltpu.VMEM)
    hbm = pl.BlockSpec(memory_space=pl.ANY)
    smem = pl.BlockSpec(memory_space=pltpu.SMEM)
    ints = pltpu.VMEM((3, pairs, LANES), jnp.int32)
    floats = pltpu.VMEM((3, pairs, LANES), F32)
    hot = pltpu.VMEM((tiles, 2 * LANES, 2 * LANES), BF16)
    out = jax.ShapeDtypeStruct((4 * tiles, LANES), F32)
    solved, left = pl.pallas_call(
        functools.partial(kernel, parts, cores),
        out_shape=(out, out),
        in_specs=[smem] + [hbm] * 6 + [vmem, smem],
        out_specs=(vmem, vmem),
        scratch_shapes=[
            pltpu.VMEM((4 * tiles, LANES), F32),
            pltpu.VMEM((4 * tiles, LANES), F32),
            pltpu.VMEM((tiles, LANES), F32),
            pltpu.VMEM((3, face_rows, LANES), F32),
            pltpu.VMEM((face_rows, LANES), jnp.int32),
            pltpu.VMEM((face_rows, LANES), jnp.int32),
            pltpu.SemaphoreType.DMA((6,)),
            ints,
            ints,
            ints,
            floats,
            floats,
            floats,
            floats,
            pltpu.VMEM((3, 3, pairs, LANES), F32),
            hot,
            pltpu.VMEM((tiles, LANES, 2 * LANES), BF16),
            pltpu.VMEM((3, 8 * pairs, LANES), F32),
            pltpu.VMEM((3, 8 * pairs, LANES), F32),
            pltpu.VMEM((2, 8 * tiles, LANES), F32),
            pltpu.VMEM((2, 8 * tiles, LANES), F32),
            pltpu.VMEM((4, tiles + 8, LANES), F32),
            pltpu.VMEM((8 * period, LANES), F32),
            pltpu.VMEM((5, tiles, LANES), F32),
            pltpu.VMEM((3, 4, tiles, LANES), F32),
            pltpu.VMEM((turns, 5 * tiles, LANES), F32),
            pltpu.VMEM((turns, 5 * tiles, LANES), F32),
            pltpu.VMEM((turns, lists // cores, 8, LANES), F32),
            pltpu.VMEM((turns, lists, 8, LANES), F32),
            pltpu.VMEM((turns + 8, 1, LANES), F32),
            pltpu.VMEM((turns, parts + 8, 1, LANES), F32),
        ]
        + [pltpu.SemaphoreType.DMA((turns,))] * 6,
        compiler_params=pltpu.CompilerParams(
            collective_id=0, has_side_effects=True, vmem_limit_bytes=56 * 1024 * 1024
        ),
    )(
        face_count,
        by_tile(flow_state),
        by_tile(source_term),
        volume_rate.reshape(tiles, LANES),
        face_normal.reshape(3, face_rows, LANES),
        face_owner.reshape(face_rows, LANES),
        face_neighbour.reshape(face_rows, LANES),
        send_list.reshape(lists, width // LANES, LANES),
        halo_count,
    )
    return by_component(solved), by_component(left)


def solution(mesh):
    in_specs = (
        P(None, "cells"),
        P(None, "cells"),
        P("cells"),
        P(None, ("cells", "faces")),
        P(("cells", "faces")),
        P(("cells", "faces")),
        P(("cells", "faces")),
        P("cells", None),
        P("cells"),
    )
    out_specs = (P(None, "cells"), P(None, "cells"))
    return jax.shard_map(body, mesh=mesh, in_specs=in_specs, out_specs=out_specs, check_vma=False)
```

```python
import functools

import jax
import jax.numpy as jnp
from jax import lax
from jax.experimental import pallas as pl
from jax.experimental.pallas import tpu as pltpu
from jax.sharding import PartitionSpec as P

ITERS = 2
LANES = 128
MESH = pl.DeviceIdType.MESH
F32 = jnp.float32
BF16 = jnp.bfloat16


def take_lanes(source, index):
    return jnp.take_along_axis(source, index, axis=1, mode="promise_in_bounds")


def split(value):
    high = value.astype(BF16).astype(F32)
    return high, value - high


def kernel(
    parts,
    cores,
    count_ref,
    flow_hbm,
    source_hbm,
    volume_hbm,
    normal_hbm,
    owner_hbm,
    neighbour_hbm,
    list_ref,
    halo_count_ref,
    solution_ref,
    residual_ref,
    flow_ref,
    source_ref,
    volume_ref,
    normal_ref,
    owner_ref,
    neighbour_ref,
    input_sem,
    own_lane,
    right_lane,
    right_kind,
    own_row,
    local_row,
    face_u,
    face_s,
    face_n,
    signed_hot,
    plain_hot,
    flux_rows,
    size_rows,
    cell_rows,
    size_cells,
    fields,
    halo_rows,
    blocks,
    vecs,
    pair_out,
    pair_in,
    halo_out,
    halo_in,
    dot_out,
    dot_in,
    pair_send,
    pair_recv,
    halo_send,
    halo_recv,
    dot_send,
    dot_recv,
):
    me = lax.axis_index("cells")
    core = lax.axis_index("faces")
    other = (core + 1) % cores
    tiles = volume_ref.shape[0]
    pairs = tiles // 2
    groups = pairs // 8
    cells = tiles * LANES
    lists = halo_in.shape[1]
    lists_here = lists // cores
    width = list_ref.shape[1] * LANES

    def fetched(number, source, target):
        copy = pltpu.make_async_copy(source, target, input_sem.at[number])
        copy.start()
        return copy

    copies = [
        fetched(0, owner_hbm, owner_ref),
        fetched(1, neighbour_hbm, neighbour_ref),
        fetched(2, flow_hbm, flow_ref),
        fetched(4, source_hbm, source_ref),
        fetched(5, volume_hbm, volume_ref),
    ]
    normals = [fetched(3, normal_hbm, normal_ref.at[pl.ds(0, 3 * pairs)])]

    barrier = pltpu.get_barrier_semaphore()
    for step in range(1, parts * cores):
        number = (me * cores + core + step) % (parts * cores)
        pl.semaphore_signal(
            barrier,
            inc=1,
            device_id={"cells": number // cores, "faces": number % cores},
            device_id_type=MESH,
        )

    lane = lax.broadcasted_iota(jnp.int32, (pairs, LANES), 1)
    pair_id = lax.broadcasted_iota(jnp.int32, (pairs, LANES), 0)
    late = lane >= LANES // 2
    count = count_ref[0]
    for copy in copies:
        copy.wait()
    for j in range(3):
        tile = 2 * pair_id + (0 if j == 0 else 1)
        if j == 1:
            tile = 2 * pair_id + late.astype(jnp.int32)
        owner = owner_ref[pl.ds(j, pairs, stride=3), :]
        beside = neighbour_ref[pl.ds(j, pairs, stride=3), :]
        live = (3 * pair_id + j) * LANES + lane < count
        is_local = beside < cells
        column = beside - tile * LANES
        column = jnp.where(column < 0, column + cells, column)
        slot = beside - cells - (tile % lists) * width
        place = jnp.where(is_local, column, slot)
        upper = place >= LANES
        own = owner - tile * LANES
        own_lane[j] = own
        right_lane[j] = jnp.where(upper, place - LANES, place)
        right_kind[j] = jnp.where(is_local, 0, 2) + upper.astype(jnp.int32)
        own_row[j] = jnp.where(live, own, -1).astype(F32)
        local_row[j] = jnp.where(live & is_local, column, -1).astype(F32)

    def start_halo(turn, field):
        row8 = lax.broadcasted_iota(jnp.int32, (8, LANES), 0)
        for i in range(lists_here):
            which = core * lists_here + i
            rows = []
            wanted = list_ref[which]
            limit = halo_count_ref[which]
            for b in range(4):
                for half in range(2):
                    cell = jnp.broadcast_to(wanted[half : half + 1], (8, LANES))
                    row = cell // LANES
                    col = cell - row * LANES
                    found = jnp.zeros((8, LANES), F32)
                    for g in range(tiles // 8):
                        got = take_lanes(field(b, g), col)
                        found = jnp.where(row == row8 + 8 * g, got, found)
                    found = jnp.sum(found, axis=0, keepdims=True)
                    used = (
                        lax.broadcasted_iota(jnp.int32, (1, LANES), 1) + half * LANES < limit
                    )
                    rows.append(jnp.where(used, found, 0.0))
            halo_out[turn, i] = jnp.concatenate(rows, axis=0)
        for i in range(lists_here):
            target = (me + (1 - 2 * core) * (i + 1) + parts) % parts
            for c in range(cores):
                pltpu.make_async_remote_copy(
                    src_ref=halo_out.at[turn, i],
                    dst_ref=halo_in.at[turn, core * lists_here + i],
                    send_sem=halo_send.at[turn],
                    recv_sem=halo_recv.at[turn],
                    device_id={"cells": target, "faces": c},
                    device_id_type=MESH,
                ).start()

    def wait_halo(turn):
        pltpu.make_async_copy(halo_in.at[turn], halo_in.at[turn], halo_recv.at[turn]).wait()
        return [halo_in[turn, k] for k in range(lists)]

    def start_pair(turn, rows):
        copy = pltpu.make_async_remote_copy(
            src_ref=pair_out.at[turn, pl.ds(0, rows)],
            dst_ref=pair_in.at[turn, pl.ds(0, rows)],
            send_sem=pair_send.at[turn],
            recv_sem=pair_recv.at[turn],
            device_id={"cells": me, "faces": other},
            device_id_type=MESH,
        )
        copy.start()
        return copy

    def start_dots(turn, partials):
        at = lax.broadcasted_iota(jnp.int32, (1, LANES), 1)
        packed = jnp.zeros((1, LANES), F32)
        for d, p in enumerate(partials):
            row = jnp.sum(p.reshape(tiles // 8, 8, LANES).sum(axis=0), axis=0, keepdims=True)
            packed = jnp.where(at == d, jnp.sum(row, axis=1, keepdims=True), packed)
        dot_out[turn] = packed
        dot_in[turn, me] = packed
        for step in range(1, parts):
            pltpu.make_async_remote_copy(
                src_ref=dot_out.at[turn],
                dst_ref=dot_in.at[turn, me],
                send_sem=dot_send.at[turn],
                recv_sem=dot_recv.at[turn],
                device_id={"cells": (me + step) % parts, "faces": core},
                device_id_type=MESH,
            ).start()

    def wait_dots(turn, number):
        part = dot_in.at[turn, pl.ds(0, parts - 1)]
        pltpu.make_async_copy(part, part, dot_recv.at[turn]).wait()
        total = dot_in[turn, 0]
        for q in range(1, parts):
            total = total + dot_in[turn, q]
        return [jnp.broadcast_to(total[:, d : d + 1], (1, LANES)) for d in range(number)]

    def put_field(values, halos):
        for b, value in enumerate(values):
            fields[b, pl.ds(0, tiles), :] = value
            fields[b, pl.ds(tiles, 1), :] = value[0:1]
        period = halo_rows.shape[0] // 8
        for t in range(period):
            halo_rows[pl.ds(t, 8, stride=period), :] = halos[t % lists]

    def sides(g, j, b):
        period = halo_rows.shape[0] // 8
        here = pl.multiple_of(g * 8, 8)
        left_at = own_lane[j, pl.ds(here, 8), :]
        right_at = right_lane[j, pl.ds(here, 8), :]
        kind = right_kind[j, pl.ds(here, 8), :]

        def of_tile(odd):
            first = 16 * g + odd
            halo_first = (16 * g) % lists + odd
            low = fields[b, pl.ds(first, 8, stride=2), :]
            high = fields[b, pl.ds(first + 1, 8, stride=2), :]
            halo_low = halo_rows[pl.ds(2 * b * period + halo_first, 8, stride=2), :]
            halo_high = halo_rows[pl.ds((2 * b + 1) * period + halo_first, 8, stride=2), :]
            left = take_lanes(low, left_at)
            right = jnp.where(
                kind < 2,
                jnp.where(kind == 0, take_lanes(low, right_at), take_lanes(high, right_at)),
                jnp.where(
                    kind == 2, take_lanes(halo_low, right_at), take_lanes(halo_high, right_at)
                ),
            )
            return left, right

        if j == 0:
            return of_tile(0)
        if j == 2:
            return of_tile(1)
        early = lax.broadcasted_iota(jnp.int32, (8, LANES), 1) < LANES // 2
        left_a, right_a = of_tile(0)
        left_b, right_b = of_tile(1)
        return jnp.where(early, left_a, left_b), jnp.where(early, right_a, right_b)

    def put_flux(ref, g, j, b, value):
        high, low = split(value)
        ref[j, pl.ds(64 * g + b, 8, stride=8), :] = high
        ref[j, pl.ds(64 * g + 4 + b, 8, stride=8), :] = low

    def tile_rows(rows_ref, u, odd):
        at = pl.ds(pl.multiple_of(u * 8, 8), 8)
        return jnp.concatenate([rows_ref[odd, at, :], rows_ref[odd + 1, at, :]], axis=1).astype(BF16)

    def added(rows, hot):
        return lax.dot_general(
            rows, hot, (((1,), (1,)), ((), ())), preferred_element_type=F32
        )

    def scatter(u):
        for odd in range(2):
            result = added(tile_rows(flux_rows, u, odd), signed_hot[2 * u + odd])
            at = pl.ds(pl.multiple_of(u * 16 + odd * 8, 8), 8)
            cell_rows[0, at, :] = result[:, :LANES]
            cell_rows[1, at, :] = result[:, LANES:]

    def scatter_size(u):
        for odd in range(2):
            rows = tile_rows(size_rows, u, odd)
            at = pl.ds(pl.multiple_of(u * 16 + odd * 8, 8), 8)
            size_cells[0, at, :] = added(rows, plain_hot[2 * u + odd])
            size_cells[1, at, :] = -added(rows, signed_hot[2 * u + odd, LANES:, :])

    def collect(cells_ref, b):
        def rows(first, side):
            return cells_ref[side, pl.ds(first, tiles, stride=8), :]

        low = rows(b, 0) + rows(4 + b, 0)
        high = rows(b, 1) + rows(4 + b, 1)
        high = jnp.concatenate([high[tiles - 1 :], high[: tiles - 1]], axis=0)
        return low + high

    def apply_matrix(turn, values, halos):
        put_field(values, halos)

        def group(g, carry):
            here = pl.multiple_of(g * 8, 8)
            for j in range(3):
                u = face_u[j, pl.ds(here, 8), :]
                s = face_s[j, pl.ds(here, 8), :]
                n = [face_n[i, j, pl.ds(here, 8), :] for i in range(3)]
                both = [sides(g, j, b) for b in range(4)]
                total = [left + right for left, right in both]
                jump = [s * (right - left) for left, right in both]
                for i in range(3):
                    put_flux(flux_rows, g, j, i, u * total[i] + n[i] * total[3] - jump[i])
                last = n[0] * total[0] + n[1] * total[1] + n[2] * total[2] - jump[3]
                put_flux(flux_rows, g, j, 3, last)
            for i in range(8):
                scatter(g * 8 + i)
            return carry

        lax.fori_loop(0, groups, group, 0)
        mine = [collect(cell_rows, b) for b in range(4)]
        for b in range(4):
            pair_out[turn, b * tiles : (b + 1) * tiles, :] = mine[b]
        copy = start_pair(turn, 4 * tiles)
        copy.wait_recv()
        volume = volume_ref[...]
        return [
            volume * values[b]
            + (
                pair_out[turn, b * tiles : (b + 1) * tiles, :]
                + pair_in[turn, b * tiles : (b + 1) * tiles, :]
            )
            for b in range(4)
        ]

    def precondition(w):
        rvd, rschur = blocks[0], blocks[1]
        n = [blocks[2 + i] for i in range(3)]
        pressure = (w[3] - (n[0] * w[0] + n[1] * w[1] + n[2] * w[2]) * rvd) * rschur
        return [(w[i] - n[i] * pressure) * rvd for i in range(3)] + [pressure]

    def load(which):
        return [vecs[which, b] for b in range(4)]

    def save(which, values):
        for b in range(4):
            vecs[which, b] = values[b]

    def dot(a, b):
        return a[0] * b[0] + a[1] * b[1] + a[2] * b[2] + a[3] * b[3]

    def saved_field(which):
        return lambda b, g: vecs[which, b, 8 * g : 8 * g + 8, :]

    PRE, IMAGE_M, TEMP = 0, 1, 2
    flow = [flow_ref[pl.ds(b, tiles, stride=4), :] for b in range(4)]
    source = [source_ref[pl.ds(b, tiles, stride=4), :] for b in range(4)]
    pl.semaphore_wait(barrier, parts * cores - 1)
    start_halo(0, lambda b, g: flow_ref[pl.ds(32 * g + b, 8, stride=4), :])
    start_dots(0, [dot(source, source)])

    cell_id = lax.broadcasted_iota(jnp.int32, (LANES, LANES), 0).astype(F32).astype(BF16)
    early_row = lax.broadcasted_iota(jnp.int32, (1, LANES), 1) < LANES // 2
    one, zero = jnp.ones((), BF16), jnp.zeros((), BF16)

    def hot_of(row):
        return jnp.where(cell_id == row.astype(BF16), one, zero)

    def build(u, carry):
        for odd in range(2):
            for half in range(2):
                j = odd + half
                own = own_row[j, pl.ds(u, 1), :]
                local = local_row[j, pl.ds(u, 1), :]
                if j == 1:
                    keep = early_row if odd == 0 else jnp.logical_not(early_row)
                    own = jnp.where(keep, own, -1.0)
                    local = jnp.where(keep, local, -1.0)
                own_hot, local_hot = hot_of(own), hot_of(local)
                lanes = slice(half * LANES, (half + 1) * LANES)
                signed_hot[2 * u + odd, :LANES, lanes] = own_hot - local_hot
                signed_hot[2 * u + odd, LANES:, lanes] = -hot_of(local - LANES)
                plain_hot[2 * u + odd, :, lanes] = own_hot + local_hot
        return carry

    lax.fori_loop(0, pairs, build, 0)
    size_rows[...] = jnp.zeros_like(size_rows)
    for copy in normals:
        copy.wait()

    put_field(flow, wait_halo(0))

    def face_terms(g, carry):
        here = pl.multiple_of(g * 8, 8)
        for j in range(3):
            n = [normal_ref[pl.ds(24 * g + j, 8, stride=3), i, :] for i in range(3)]
            both = [sides(g, j, b) for b in range(3)]
            total = [left + right for left, right in both]
            u = 0.5 * (n[0] * total[0] + n[1] * total[1] + n[2] * total[2])
            s = jnp.abs(u) + 2.0 * jnp.sqrt(n[0] * n[0] + n[1] * n[1] + n[2] * n[2])
            u, s = 0.5 * u, 0.5 * s
            n = [0.5 * n[i] for i in range(3)]
            face_u[j, pl.ds(here, 8), :] = u
            face_s[j, pl.ds(here, 8), :] = s
            put_flux(flux_rows, g, j, 0, u)
            for i in range(3):
                face_n[i, j, pl.ds(here, 8), :] = n[i]
                put_flux(flux_rows, g, j, 1 + i, n[i])
            put_flux(size_rows, g, j, 0, s)
        for i in range(8):
            scatter(g * 8 + i)
            scatter_size(g * 8 + i)
        return carry

    lax.fori_loop(0, groups, face_terms, 0)
    for b in range(4):
        pair_out[0, b * tiles : (b + 1) * tiles, :] = collect(cell_rows, b)
    pair_out[0, 4 * tiles : 5 * tiles, :] = collect(size_cells, 0)
    start_pair(0, 5 * tiles).wait_recv()
    sums = [
        pair_out[0, b * tiles : (b + 1) * tiles, :] + pair_in[0, b * tiles : (b + 1) * tiles, :]
        for b in range(5)
    ]
    volume = volume_ref[...]
    rvd = 1.0 / (volume + sums[0] + sums[4])
    coupling = sums[1:4]
    norm = coupling[0] * coupling[0] + coupling[1] * coupling[1] + coupling[2] * coupling[2]
    blocks[0] = rvd
    blocks[1] = 1.0 / (volume + sums[4] - norm * rvd)
    for i in range(3):
        blocks[2 + i] = coupling[i]

    def combine(a, scale, b):
        return [x + scale * y for x, y in zip(a, b)]

    residual = source
    direction = source
    pre_dir = precondition(direction)
    save(PRE, pre_dir)
    start_halo(1, saved_field(PRE))
    (rho,) = wait_dots(0, 1)
    halo_dir = wait_halo(1)
    halo_res = halo_dir
    answer = None
    for iteration in range(ITERS):
        final = iteration + 1 == ITERS
        turn = 1 + 2 * iteration
        image = apply_matrix(turn, pre_dir, halo_dir)
        start_dots(turn, [dot(source, image)])
        pre_image = precondition(image)
        save(IMAGE_M, pre_image)
        start_halo(turn + 1, saved_field(IMAGE_M))
        pre_res = pre_dir if iteration == 0 else precondition(residual)
        (shadow_image,) = wait_dots(turn, 1)
        alpha = rho / shadow_image
        middle = combine(residual, -alpha, image)
        pre_mid = combine(pre_res, -alpha, pre_image)
        halo_image = wait_halo(turn + 1)
        halo_mid = combine(halo_res, -alpha, halo_image)
        second = apply_matrix(turn + 1, pre_mid, halo_mid)
        start_dots(
            turn + 1,
            [dot(second, middle), dot(second, second), dot(source, middle), dot(source, second)],
        )
        if not final:
            pre_second = precondition(second)
            save(TEMP, pre_second)
            start_halo(turn + 2, saved_field(TEMP))
        second_mid, second_sq, shadow_mid, shadow_second = wait_dots(turn + 1, 4)
        omega = second_mid / second_sq
        step = combine([alpha * v for v in pre_dir], omega, pre_mid)
        answer = step if answer is None else [a + s for a, s in zip(answer, step)]
        residual = combine(middle, -omega, second)
        if not final:
            rho_next = shadow_mid - omega * shadow_second
            beta = rho_next / rho * (alpha / omega)
            rho = rho_next
            direction = combine(residual, beta, combine(direction, -omega, image))
            pre_dir = precondition(direction)
            halo_second = wait_halo(turn + 2)
            halo_res = combine(halo_mid, -omega, halo_second)
            halo_dir = combine(halo_res, beta, combine(halo_dir, -omega, halo_image))
    for b in range(4):
        solution_ref[pl.ds(b, tiles, stride=4), :] = answer[b]
        residual_ref[pl.ds(b, tiles, stride=4), :] = residual[b]

    for turn in range(halo_in.shape[0]):
        pltpu.make_async_copy(halo_in.at[turn], halo_in.at[turn], halo_send.at[turn]).wait()
    for turn in range(pair_in.shape[0]):
        part = pair_out.at[turn, pl.ds(0, (5 if turn == 0 else 4) * tiles)]
        pltpu.make_async_copy(part, part, pair_send.at[turn]).wait()
        part = dot_in.at[turn, pl.ds(0, parts - 1)]
        pltpu.make_async_copy(part, part, dot_send.at[turn]).wait()


def body(
    flow_state,
    source_term,
    volume_rate,
    face_normal,
    face_owner,
    face_neighbour,
    face_count,
    send_list,
    halo_count,
):
    parts = lax.axis_size("cells")
    cores = lax.axis_size("faces")
    cells = flow_state.shape[1]
    tiles = cells // LANES
    pairs = tiles // 2
    face_rows = face_owner.shape[0] // LANES
    lists, width = send_list.shape
    period = -(-(lists + 16) // 8) * 8
    turns = 1 + 2 * ITERS

    def by_tile(field):
        return field.reshape(4, tiles, LANES).transpose(1, 0, 2).reshape(4 * tiles, LANES)

    def by_component(field):
        return field.reshape(tiles, 4, LANES).transpose(1, 0, 2).reshape(4, cells)

    vmem = pl.BlockSpec(memory_space=pltpu.VMEM)
    hbm = pl.BlockSpec(memory_space=pl.ANY)
    smem = pl.BlockSpec(memory_space=pltpu.SMEM)
    ints = pltpu.VMEM((3, pairs, LANES), jnp.int32)
    floats = pltpu.VMEM((3, pairs, LANES), F32)
    hot = pltpu.VMEM((tiles, 2 * LANES, 2 * LANES), BF16)
    out = jax.ShapeDtypeStruct((4 * tiles, LANES), F32)
    solved, left = pl.pallas_call(
        functools.partial(kernel, parts, cores),
        out_shape=(out, out),
        in_specs=[smem] + [hbm] * 6 + [vmem, smem],
        out_specs=(vmem, vmem),
        scratch_shapes=[
            pltpu.VMEM((4 * tiles, LANES), F32),
            pltpu.VMEM((4 * tiles, LANES), F32),
            pltpu.VMEM((tiles, LANES), F32),
            pltpu.VMEM((face_rows + 8, 3, LANES), F32),
            pltpu.VMEM((face_rows, LANES), jnp.int32),
            pltpu.VMEM((face_rows, LANES), jnp.int32),
            pltpu.SemaphoreType.DMA((6,)),
            ints,
            ints,
            ints,
            floats,
            floats,
            floats,
            floats,
            pltpu.VMEM((3, 3, pairs, LANES), F32),
            hot,
            pltpu.VMEM((tiles, LANES, 2 * LANES), BF16),
            pltpu.VMEM((3, 8 * pairs, LANES), F32),
            pltpu.VMEM((3, 8 * pairs, LANES), F32),
            pltpu.VMEM((2, 8 * tiles, LANES), F32),
            pltpu.VMEM((2, 8 * tiles, LANES), F32),
            pltpu.VMEM((4, tiles + 8, LANES), F32),
            pltpu.VMEM((8 * period, LANES), F32),
            pltpu.VMEM((5, tiles, LANES), F32),
            pltpu.VMEM((3, 4, tiles, LANES), F32),
            pltpu.VMEM((turns, 5 * tiles, LANES), F32),
            pltpu.VMEM((turns, 5 * tiles, LANES), F32),
            pltpu.VMEM((turns, lists // cores, 8, LANES), F32),
            pltpu.VMEM((turns, lists, 8, LANES), F32),
            pltpu.VMEM((turns + 8, 1, LANES), F32),
            pltpu.VMEM((turns, parts + 8, 1, LANES), F32),
        ]
        + [pltpu.SemaphoreType.DMA((turns,))] * 6,
        compiler_params=pltpu.CompilerParams(
            collective_id=0, has_side_effects=True, vmem_limit_bytes=56 * 1024 * 1024
        ),
    )(
        face_count,
        by_tile(flow_state),
        by_tile(source_term),
        volume_rate.reshape(tiles, LANES),
        face_normal.reshape(3, face_rows, LANES).transpose(1, 0, 2),
        face_owner.reshape(face_rows, LANES),
        face_neighbour.reshape(face_rows, LANES),
        send_list.reshape(lists, width // LANES, LANES),
        halo_count,
    )
    return by_component(solved), by_component(left)


def solution(mesh):
    in_specs = (
        P(None, "cells"),
        P(None, "cells"),
        P("cells"),
        P(None, ("cells", "faces")),
        P(("cells", "faces")),
        P(("cells", "faces")),
        P(("cells", "faces")),
        P("cells", None),
        P("cells"),
    )
    out_specs = (P(None, "cells"), P(None, "cells"))
    return jax.shard_map(body, mesh=mesh, in_specs=in_specs, out_specs=out_specs, check_vma=False)
```
